32 devices in a mesh: dp: 4 (over y, x), tensor: 2 (over core), precond: 4 (over z).
Axes of the slice: x: 2, y: 2, z: 4, core: 2. Of those that a mesh axis runs over, the one named last changes fastest.
Arguments:
- tokens: bfloat16 [512, 8192], P('dp', 'tensor'), may hold values from -6 to 6
- gain: bfloat16 [8192], P('tensor'), may hold values from 0.099609375 to 1.8984375
- cotangent: bfloat16 [512, 12288], P('dp', 'precond'), may hold values from -6 to 6
Outputs:
- preconditioner: float32 [8, 1024, 1024], P('tensor', ('dp', 'precond'))
The draws below stay inside these ranges and needn't reach their ends.
All inputs are finite; a program needn't handle non-finite values.
Results may differ from the reference program's by a relative error of at most 0.00089.
Values sent between devices are 32-bit elements; how exact they have to be, the bound alone decides.
No kernel may reach another device: no remote copies, remote signals or barrier semaphores. Data moves between devices by JAX's collectives and lax.ppermute only.
A program may use at most 128 MiB of HBM per device.

```python
import jax
import jax.numpy as jnp
from jax import lax

D = 8192
FFW = 12288
BLK = 1024
TOKENS = 512


def draw_cotangent(key, part):
    key_normal = jax.random.fold_in(jax.random.fold_in(key, 17), 0)
    sample = jnp.clip(jax.random.normal(key_normal, (TOKENS, FFW), jnp.float32), -6.0, 6.0)
    return sample.astype(jnp.bfloat16)


def levels(own_key, shape, pieces, low, high):
    level = 1.0
    for axis_at, blocks in pieces:
        heights = jax.random.uniform(jax.random.fold_in(jax.random.fold_in(own_key, 6), axis_at), (blocks,), jnp.float32, low / len(pieces), high / len(pieces))
        level = level * jnp.repeat(jnp.exp(heights), shape[axis_at] // blocks).reshape((-1,) + (1,) * (len(shape) - 1 - axis_at))
    return level


def normal_values(stream_key, dims, scale, bound, cuts=(), held_as=jnp.bfloat16):
    level = levels(stream_key, dims, cuts, -0.22, 0.18) if cuts else 1.0
    entries = jax.random.normal(stream_key, dims, jnp.float32) * scale * level
    return jnp.minimum(jnp.maximum(entries, -bound), bound).astype(held_as)


def setup_inputs(seed: int = 0) -> dict:
    seeds = jax.random.split(jax.random.key(seed), 4)
    tokens = normal_values(seeds[0], (TOKENS, D), 1.0, 6.0, ((0, 4), (1, 2)))
    gain = jnp.clip(1.0 + 0.18 * jax.random.normal(seeds[1], (D,), jnp.float32), 0.099609375, 1.8984375).astype(jnp.bfloat16)
    cotangent = draw_cotangent(jax.random.fold_in(seeds[3], 71), 0)
    return dict(tokens=tokens, gain=gain, cotangent=cotangent)


highest = lax.Precision.HIGHEST
epsilon = 1e-06
damping = 0.01

def precondition_block(block):
    identity = jnp.eye(BLK, dtype=jnp.float32)
    statistic = jnp.dot(block, block.T, precision=highest) + damping * identity
    scaling = 2.0 * jnp.trace(statistic) / BLK
    start_iterate = statistic / scaling
    factor_one = (5.0 * identity - start_iterate) / 4.0
    power_two = jnp.dot(factor_one, factor_one, precision=highest)
    power_four = jnp.dot(power_two, power_two, precision=highest)
    next_iterate = jnp.dot(power_four, start_iterate, precision=highest)
    factor_two = (5.0 * identity - next_iterate) / 4.0
    return jnp.power(scaling, -0.25) * jnp.dot(factor_one, factor_two, precision=highest)

def reference(tokens, gain, cotangent):
    values = tokens.astype(jnp.float32)
    mean_square = lax.optimization_barrier(jnp.mean(values * values, axis=1, keepdims=True))
    normed = (values * lax.rsqrt(mean_square + epsilon) * gain.astype(jnp.float32)).astype(jnp.bfloat16)
    gradient = jnp.dot(normed.T, cotangent, preferred_element_type=jnp.float32) / TOKENS
    blocks = gradient.reshape(D // BLK, BLK, FFW)
    return lax.map(precondition_block, blocks)
```

```python
import functools

import jax
import jax.numpy as jnp
from jax import lax
from jax.experimental import pallas as pl
from jax.experimental.pallas import tpu as pltpu
from jax.sharding import PartitionSpec as P

BLK = 1024

epsilon = 1e-06
damping = 0.01

f32 = jnp.float32
bf16 = jnp.bfloat16
VMEM = pl.BlockSpec(memory_space=pltpu.VMEM)
SMEM = pl.BlockSpec(memory_space=pltpu.SMEM)


def shift(value, axis, by):
    size = lax.axis_size(axis)
    return lax.ppermute(value, axis, [(i, (i + by) % size) for i in range(size)])


def call(kernel, outs, *operands, scratch=(), flops=0):
    moved = sum(a.size * a.dtype.itemsize for a in (*operands, *outs))
    return pl.pallas_call(
        kernel,
        out_shape=list(outs),
        in_specs=[SMEM] + [VMEM] * (len(operands) - 1),
        out_specs=[VMEM] * len(outs),
        scratch_shapes=list(scratch),
        cost_estimate=pl.CostEstimate(flops=flops, bytes_accessed=moved, transcendentals=0),
    )(*operands)


def nt(left, right):
    return lax.dot_general(left, right, (((1,), (1,)), ((), ())), preferred_element_type=f32)


def nn(left, right):
    return lax.dot_general(left, right, (((1,), (0,)), ((), ())), preferred_element_type=f32)


def halves(value):
    high = value.astype(bf16)
    return high, (value - high.astype(f32)).astype(bf16)


def product(left, right):
    return nn(left[0], right[0]) + (nn(left[0], right[1]) + nn(left[1], right[0]))


def gram_kernel(dp, nten, where, own, *refs):
    received, outs, whole, packed = refs[: dp - 1], refs[dp - 1 : -2], refs[-2], refs[-1]
    me, ten = where[0], where[1]
    size = own.shape[0]
    whole[pl.ds(pl.multiple_of(me * size, size), size)] = own[...].astype(bf16)
    for by, piece in enumerate(received, 1):
        source = lax.rem(me + dp - by, dp)
        whole[pl.ds(pl.multiple_of(source * size, size), size)] = piece[...].astype(bf16)
    at = 0
    for i in range(dp):
        rows = nt(whole[i * size : (i + 1) * size], whole[i * size :])
        for j in range(dp - i):
            packed[at * size : (at + 1) * size] = rows[:, j * size : (j + 1) * size]
            at += 1
    if at * size < packed.shape[0]:
        packed[at * size :] = jnp.zeros((packed.shape[0] - at * size, size), f32)
    count = outs[0].shape[0]
    for by, out in enumerate(outs):
        target = lax.rem(ten + by, nten)
        out[...] = packed[pl.ds(pl.multiple_of(target * count, 8), count)]


def split_kernel(axis_at, terms, where, *refs):
    parts, outs, total = refs[:terms], refs[terms:-1], refs[-1]
    value = parts[0][...]
    for part in parts[1:]:
        value = value + part[...]
    total[...] = value
    size, count = len(outs), outs[0].shape[0]
    for by, out in enumerate(outs):
        target = lax.rem(where[axis_at] + by, size)
        out[...] = total[pl.ds(pl.multiple_of(target * count, 8), count)]


def join_kernel(axis_at, where, *refs):
    parts, out = refs[:-1], refs[-1]
    size, count = len(parts), parts[0].shape[0]
    for by, part in enumerate(parts):
        source = lax.rem(where[axis_at] + size - by, size)
        out[pl.ds(pl.multiple_of(source * count, 8), count)] = part[...]


def normed_kernel(dp, nb, npre, where, own, *refs):
    received, normed, gram, columns = refs[: dp - 1], refs[-3], refs[-2], refs[-1]
    me, pre = where[0], where[2]
    size = own.shape[0]
    normed[pl.ds(pl.multiple_of(me * size, size), size)] = own[...].astype(bf16)
    for by, piece in enumerate(received, 1):
        source = lax.rem(me + dp - by, dp)
        normed[pl.ds(pl.multiple_of(source * size, size), size)] = piece[...].astype(bf16)
    gram[...] = nt(normed[...], normed[...])
    select = output_rows(dp, nb, npre, me, pre, columns.shape[0], normed.shape[1])
    columns[...] = nt(select.astype(bf16), normed[...]).astype(bf16)


def output_rows(dp, nb, npre, me, pre, count, width):
    each = width // (dp * npre)
    made = lax.broadcasted_iota(jnp.int32, (count, width), 0)
    column = lax.broadcasted_iota(jnp.int32, (count, width), 1)
    target = lax.rem(me, dp // nb) * nb + made // each
    return ((target * npre + pre) * each + lax.rem(made, each) == column).astype(f32)


def root_kernel(dp, nb, npre, nten, where, normed, gram, columns, *refs):
    pieces, out, packed, inner = refs[:nten], refs[nten], refs[nten + 1], refs[nten + 2]
    me, ten, pre = where[0], where[1], where[2]
    count = pieces[0].shape[0]
    for by, piece in enumerate(pieces):
        source = lax.rem(ten + nten - by, nten)
        packed[pl.ds(pl.multiple_of(source * count, 8), count)] = piece[...]
    total = normed.shape[0]
    size, at = total // dp, 0
    for i in range(dp):
        for j in range(i, dp):
            tile = packed[at * size : (at + 1) * size]
            inner[i * size : (i + 1) * size, j * size : (j + 1) * size] = tile
            if j > i:
                inner[j * size : (j + 1) * size, i * size : (i + 1) * size] = tile.T
            at += 1
    tokens_gram = gram[...]
    width = normed.shape[1]
    power = jnp.sum(jnp.sum(inner[...] * tokens_gram, axis=1, keepdims=True), axis=0, keepdims=True)
    scaling = 2.0 * (power / (float(total) * float(total)) / width + damping)
    shared = 1.0 / (scaling * (float(total) * float(total)))
    damp = damping / scaling
    base = (5.0 - damp) / 4.0
    core = halves(inner[...] * shared)
    mixed = halves(product(halves(tokens_gram), core))
    left = columns[...]
    rows = nn(left, core[0]) + nn(left, core[1])

    def step(value, weight):
        return base * value - 0.25 * product(halves(value), mixed) + weight * rows

    weight = 0.25 * damp
    value = step(-rows, weight)
    for _ in range(3):
        weight = weight * base
        value = step(value, weight)
    weight = weight * base
    value = step(value, weight - 1.25)
    root = lax.rsqrt(jnp.sqrt(scaling))
    value = halves(value * (0.25 * root))
    alone = (5.0 * base - damp * base * base * base * base * base) * 0.25 * root
    made = nn(value[0], normed[...]) + nn(value[1], normed[...])
    select = output_rows(dp, nb, npre, me, pre, made.shape[0], width)
    out[...] = made + alone * select


def body(tokens, gain, cotangent):
    dp, nten, npre = (lax.axis_size(name) for name in ("dp", "tensor", "precond"))
    me, ten, pre = (lax.axis_index(name) for name in ("dp", "tensor", "precond"))
    where = jnp.stack([me, ten, pre]).astype(jnp.int32)
    size, width = tokens.shape
    total = size * dp
    nb = width // BLK
    share = dp // nb
    assert nb * BLK == width and share * nb == dp
    hidden = cotangent.shape[1] // (nten * dp)
    assert hidden * nten * dp == cotangent.shape[1]

    def cotangent_part(to):
        return lax.dynamic_slice_in_dim(cotangent, (ten * dp + to) * hidden, hidden, 1)

    cotangents = [cotangent_part(me)]
    for by in range(1, dp):
        cotangents.append(shift(cotangent_part(lax.rem(me + by, dp)).astype(f32), "dp", by))

    values = tokens.astype(f32)
    square = jnp.sum(values * values, axis=1)[None, :]
    square = square + sum(shift(square, "tensor", by) for by in range(1, nten))
    inverse = lax.rsqrt(square[0][:, None] / (width * nten) + epsilon)

    def normed_part(to):
        at = (to // share) * BLK
        part = lax.dynamic_slice_in_dim(tokens, at, BLK, 1).astype(f32)
        scale = lax.dynamic_slice_in_dim(gain, at, BLK, 0).astype(f32)
        return part * inverse * scale

    normed_parts = [normed_part(me)]
    for by in range(1, dp):
        normed_parts.append(shift(normed_part(lax.rem(me + by, dp)), "dp", by))

    tiles = dp * (dp + 1) // 2
    piece = -(-tiles * size // (nten * npre * 8)) * 8
    packed = jax.ShapeDtypeStruct((nten * npre * piece, size), f32)
    part = jax.ShapeDtypeStruct((npre * piece, size), f32)
    small = jax.ShapeDtypeStruct((piece, size), f32)
    parts = call(
        functools.partial(gram_kernel, dp, nten),
        [part] * nten,
        where,
        *cotangents,
        scratch=[pltpu.VMEM((total, hidden), bf16), pltpu.VMEM(packed.shape, f32)],
        flops=tiles * size * size * hidden * 2,
    )
    parts = [parts[0]] + [shift(parts[by], "tensor", by) for by in range(1, nten)]
    pieces = call(
        functools.partial(split_kernel, 2, nten),
        [small] * npre,
        where,
        *parts,
        scratch=[pltpu.VMEM(part.shape, f32)],
    )
    summed = pieces[0] + sum(shift(pieces[by], "precond", by) for by in range(1, npre))
    summed = summed + sum(shift(summed, "dp", by) for by in range(1, dp))
    pieces = [summed] + [shift(summed, "precond", by) for by in range(1, npre)]
    (joined,) = call(functools.partial(join_kernel, 2), [part], where, *pieces)
    parts = [joined] + [shift(joined, "tensor", by) for by in range(1, nten)]

    made = nb * (BLK // (dp * npre))
    normed, gram, columns = call(
        functools.partial(normed_kernel, dp, nb, npre),
        [
            jax.ShapeDtypeStruct((total, BLK), bf16),
            jax.ShapeDtypeStruct((total, total), f32),
            jax.ShapeDtypeStruct((made, total), bf16),
        ],
        where,
        *normed_parts,
        flops=2 * total * total * BLK + 2 * made * BLK * total,
    )
    (rows,) = call(
        functools.partial(root_kernel, dp, nb, npre, nten),
        [jax.ShapeDtypeStruct((made, BLK), f32)],
        where,
        normed,
        gram,
        columns,
        *parts,
        scratch=[pltpu.VMEM(packed.shape, f32), pltpu.VMEM((total, total), f32)],
        flops=2 * total * total * (3 * total + 17 * made),
    )
    rows = rows.reshape(nb, made // nb, BLK)
    if share == 1:
        return lax.all_to_all(rows, "dp", 0, 0, tiled=True)
    block, member = me // share, lax.rem(me, share)
    result = jnp.zeros_like(rows)
    for by in range(nb):
        sent = lax.dynamic_index_in_dim(rows, lax.rem(block + by, nb), 0, True)
        pairs = [(b * share + m, m * nb + (b + by) % nb) for b in range(nb) for m in range(share)]
        if any(a != b for a, b in pairs):
            sent = lax.ppermute(sent, "dp", pairs)
        source = lax.rem(lax.rem(me, nb) + nb - by, nb)
        result = lax.dynamic_update_slice_in_dim(result, sent, source, 0)
    return result


def solution(mesh):
    in_specs = (P("dp", "tensor"), P("tensor"), P("dp", "precond"))
    out_specs = P("tensor", ("dp", "precond"), None)
    return jax.shard_map(body, mesh=mesh, in_specs=in_specs, out_specs=out_specs, check_vma=False)
```

```python
import functools

import jax
import jax.numpy as jnp
from jax import lax
from jax.experimental import pallas as pl
from jax.experimental.pallas import tpu as pltpu
from jax.sharding import PartitionSpec as P

BLK = 1024

epsilon = 1e-06
damping = 0.01

f32 = jnp.float32
bf16 = jnp.bfloat16
VMEM = pl.BlockSpec(memory_space=pltpu.VMEM)
SMEM = pl.BlockSpec(memory_space=pltpu.SMEM)


def swap(value, axis, by):
    size = lax.axis_size(axis)
    return lax.ppermute(value, axis, [(i, i ^ by) for i in range(size)])


def call(kernel, outs, *operands, scratch=(), flops=0):
    moved = sum(a.size * a.dtype.itemsize for a in (*operands, *outs))
    return pl.pallas_call(
        kernel,
        out_shape=list(outs),
        in_specs=[SMEM] + [VMEM] * (len(operands) - 1),
        out_specs=[VMEM] * len(outs),
        scratch_shapes=list(scratch),
        compiler_params=pltpu.CompilerParams(vmem_limit_bytes=24 * 2**20),
        cost_estimate=pl.CostEstimate(flops=flops, bytes_accessed=moved, transcendentals=0),
    )(*operands)


def nt(left, right):
    return lax.dot_general(left, right, (((1,), (1,)), ((), ())), preferred_element_type=f32)


def nn(left, right):
    return lax.dot_general(left, right, (((1,), (0,)), ((), ())), preferred_element_type=f32)


def halves(value):
    high = value.astype(bf16)
    return high, (value - high.astype(f32)).astype(bf16)


def product(left, right):
    return nn(left[0], right[0]) + (nn(left[0], right[1]) + nn(left[1], right[0]))


def rows_at(index, count):
    return pl.ds(pl.multiple_of(index * count, 8), count)


def gram_kernel(nten, npre, where, own, *refs):
    received, outs, whole, packed = refs[: -nten - 2], refs[-nten - 2 : -2], refs[-2], refs[-1]
    me, ten, pre = where[0], where[1], where[2]
    size, dp = own.shape[0], len(received) + 1
    whole[rows_at(me, size)] = own[...].astype(bf16)
    for by, piece in enumerate(received, 1):
        whole[rows_at(me ^ by, size)] = piece[...].astype(bf16)
    at = 0
    for i in range(dp):
        rows = nt(whole[i * size : (i + 1) * size], whole[i * size :])
        for j in range(dp - i):
            packed[at * size : (at + 1) * size] = rows[:, j * size : (j + 1) * size]
            at += 1
    if at * size < packed.shape[0]:
        packed[at * size :] = jnp.zeros((packed.shape[0] - at * size, size), f32)
    count = packed.shape[0] // (nten * npre)
    for to, out in enumerate(outs):
        for by in range(npre):
            out[by * count : (by + 1) * count] = packed[rows_at((ten ^ to) * npre + (pre ^ by), count)]


def output_rows(dp, nb, npre, me, pre, count, width):
    each, share = width // (dp * npre), dp // nb
    made = lax.broadcasted_iota(jnp.int32, (count, width), 0)
    column = lax.broadcasted_iota(jnp.int32, (count, width), 1)
    target = lax.rem(me, share) * nb + ((me // share) ^ (made // each))
    return ((target * npre + pre) * each + lax.rem(made, each) == column).astype(f32)


def normed_kernel(nb, npre, where, own, *refs):
    received, (normed, high, low, columns) = refs[:-4], refs[-4:]
    me, pre = where[0], where[2]
    size, dp = own.shape[0], len(received) + 1
    normed[rows_at(me, size)] = own[...].astype(bf16)
    for by, piece in enumerate(received, 1):
        normed[rows_at(me ^ by, size)] = piece[...].astype(bf16)
    high[...], low[...] = halves(nt(normed[...], normed[...]))
    select = output_rows(dp, nb, npre, me, pre, columns.shape[0], normed.shape[1])
    columns[...] = nt(select.astype(bf16), normed[...]).astype(bf16)


def root_kernel(dp, nb, npre, nten, where, normed, high, low, columns, *refs):
    pieces, outs, packed, inner = refs[: nten * npre], refs[nten * npre : -2], refs[-2], refs[-1]
    me, ten, pre = where[0], where[1], where[2]
    for at, piece in enumerate(pieces):
        packed[rows_at((ten ^ at // npre) * npre + (pre ^ at % npre), piece.shape[0])] = piece[...]
    total, width = normed.shape
    size, at = total // dp, 0
    for i in range(dp):
        for j in range(i, dp):
            tile = packed[at * size : (at + 1) * size]
            inner[i * size : (i + 1) * size, j * size : (j + 1) * size] = tile
            if j > i:
                inner[j * size : (j + 1) * size, i * size : (i + 1) * size] = tile.T
            at += 1
    tokens_gram = high[...], low[...]
    both = inner[...] * (tokens_gram[0].astype(f32) + tokens_gram[1].astype(f32))
    power = jnp.sum(jnp.sum(both, axis=0, keepdims=True), axis=1, keepdims=True)
    scaling = 2.0 * (power / (float(total) * float(total)) / width + damping)
    damp = damping / scaling
    base = (5.0 - damp) / 4.0
    core = halves(inner[...] * (1.0 / (scaling * (float(total) * float(total)))))
    mixed = halves(product(tokens_gram, core))
    rows = nn(columns[...], core[0]) + nn(columns[...], core[1])

    def step(value, weight):
        return base * value - 0.25 * product(halves(value), mixed) + weight * rows

    weight = 0.25 * damp
    value = step(-rows, weight)
    for _ in range(3):
        weight = weight * base
        value = step(value, weight)
    weight = weight * base
    value = step(value, weight - 1.25)
    root = lax.rsqrt(jnp.sqrt(scaling))
    value = halves(value * (0.25 * root))
    alone = (5.0 * base - damp * base * base * base * base * base) * 0.25 * root
    made = nn(value[0], normed[...]) + nn(value[1], normed[...])
    made = made + alone * output_rows(dp, nb, npre, me, pre, made.shape[0], width)
    each = outs[0].shape[0]
    for by, out in enumerate(outs):
        out[...] = made[by * each : (by + 1) * each]


def program(tokens, gain, cotangent):
    dp, nten, npre = (lax.axis_size(name) for name in ("dp", "tensor", "precond"))
    me, ten, pre = (lax.axis_index(name) for name in ("dp", "tensor", "precond"))
    where = jnp.stack([me, ten, pre]).astype(jnp.int32)
    size, width = tokens.shape
    total = size * dp
    nb = width // BLK
    share = dp // nb
    assert nb * BLK == width and share * nb == dp
    assert all(n & (n - 1) == 0 for n in (dp, nten, npre))
    hidden = cotangent.shape[1] // (nten * dp)
    assert hidden * nten * dp == cotangent.shape[1]

    def cotangent_part(to):
        return lax.dynamic_slice_in_dim(cotangent, (ten * dp + to) * hidden, hidden, 1)

    cotangents = [swap(cotangent_part(me ^ by).astype(f32), "dp", by) for by in range(1, dp)]
    cotangents = [cotangent_part(me)] + cotangents

    values = tokens.astype(f32)
    square = jnp.sum(values * values, axis=1)[None, :]
    square = square + sum(swap(square, "tensor", by) for by in range(1, nten))
    inverse = lax.rsqrt(square[0][:, None] / (width * nten) + epsilon)

    def normed_part(to):
        at = (to // share) * BLK
        part = lax.dynamic_slice_in_dim(tokens, at, BLK, 1).astype(f32)
        scale = lax.dynamic_slice_in_dim(gain, at, BLK, 0).astype(f32)
        return part * inverse * scale

    normed_parts = [swap(normed_part(me ^ by), "dp", by) for by in range(1, dp)]
    normed_parts = [normed_part(me)] + normed_parts

    tiles = dp * (dp + 1) // 2
    piece = -(-tiles * size // (nten * npre * 8)) * 8
    packed = pltpu.VMEM((nten * npre * piece, size), f32)
    part = jax.ShapeDtypeStruct((npre * piece, size), f32)
    parts = call(
        functools.partial(gram_kernel, nten, npre),
        [part] * nten,
        where,
        *cotangents,
        scratch=[pltpu.VMEM((total, hidden), bf16), packed],
        flops=tiles * size * size * hidden * 2,
    )
    part = parts[0] + sum(swap(parts[to], "tensor", to) for to in range(1, nten))
    summed = part[:piece] + sum(
        swap(part[by * piece : (by + 1) * piece], "precond", by) for by in range(1, npre)
    )
    summed = summed + sum(swap(summed, "dp", by) for by in range(1, dp))
    pieces = [summed] + [swap(summed, "precond", by) for by in range(1, npre)]
    pieces = pieces + [swap(one, "tensor", to) for to in range(1, nten) for one in pieces]

    each = BLK // (dp * npre)
    made = nb * each
    normed, high, low, columns = call(
        functools.partial(normed_kernel, nb, npre),
        [
            jax.ShapeDtypeStruct((total, BLK), bf16),
            jax.ShapeDtypeStruct((total, total), bf16),
            jax.ShapeDtypeStruct((total, total), bf16),
            jax.ShapeDtypeStruct((made, total), bf16),
        ],
        where,
        *normed_parts,
        flops=2 * total * total * BLK + 2 * made * BLK * total,
    )
    rows = call(
        functools.partial(root_kernel, dp, nb, npre, nten),
        [jax.ShapeDtypeStruct((each, BLK), f32)] * nb,
        where,
        normed,
        high,
        low,
        columns,
        *pieces,
        scratch=[packed, pltpu.VMEM((total, total), f32)],
        flops=2 * total * total * (3 * total + 17 * made),
    )
    result = jnp.zeros((nb, each, BLK), f32)
    for by in range(nb):
        pairs = [(b * share + m, m * nb + (b ^ by)) for b in range(nb) for m in range(share)]
        sent = rows[by]
        if any(a != b for a, b in pairs):
            sent = lax.ppermute(sent, "dp", pairs)
        result = lax.dynamic_update_slice_in_dim(result, sent[None], lax.rem(me, nb) ^ by, 0)
    return result


def solution(mesh):
    in_specs = (P("dp", "tensor"), P("tensor"), P("dp", "precond"))
    out_specs = P("tensor", ("dp", "precond"), None)
    return jax.shard_map(program, mesh=mesh, in_specs=in_specs, out_specs=out_specs, check_vma=False)
```

```python
import functools

import jax
import jax.numpy as jnp
from jax import lax
from jax.experimental import pallas as pl
from jax.experimental.pallas import tpu as pltpu
from jax.sharding import PartitionSpec as P

BLK = 1024


epsilon = 1e-06
damping = 0.01

f32 = jnp.float32
bf16 = jnp.bfloat16
VMEM = pl.BlockSpec(memory_space=pltpu.VMEM)
SMEM = pl.BlockSpec(memory_space=pltpu.SMEM)


def swap(value, axis, by):
    size = lax.axis_size(axis)
    return lax.ppermute(value, axis, [(i, i ^ by) for i in range(size)])


def call(kernel, outs, *operands, scratch=(), flops=0):
    moved = sum(a.size * a.dtype.itemsize for a in (*operands, *outs))
    return pl.pallas_call(
        kernel,
        out_shape=list(outs),
        in_specs=[SMEM] + [VMEM] * (len(operands) - 1),
        out_specs=[VMEM] * len(outs),
        scratch_shapes=list(scratch),
        compiler_params=pltpu.CompilerParams(vmem_limit_bytes=24 * 2**20),
        cost_estimate=pl.CostEstimate(flops=flops, bytes_accessed=moved, transcendentals=0),
    )(*operands)


def nt(left, right):
    return lax.dot_general(left, right, (((1,), (1,)), ((), ())), preferred_element_type=f32)


def nn(left, right):
    return lax.dot_general(left, right, (((1,), (0,)), ((), ())), preferred_element_type=f32)


def halves(value):
    high = value.astype(bf16)
    return high, (value - high.astype(f32)).astype(bf16)


def product(left, right):
    return nn(left[0], right[0]) + (nn(left[0], right[1]) + nn(left[1], right[0]))


def rows_at(index, count):
    return pl.ds(pl.multiple_of(index * count, 8), count)


def gram_kernel(nten, npre, where, own, *refs):
    received, outs, whole, packed = refs[: -nten - 2], refs[-nten - 2 : -2], refs[-2], refs[-1]
    me, ten, pre = where[0], where[1], where[2]
    size, dp = own.shape[0], len(received) + 1
    whole[rows_at(me, size)] = own[...].astype(bf16)
    for by, piece in enumerate(received, 1):
        whole[rows_at(me ^ by, size)] = piece[...].astype(bf16)
    at = 0
    for i in range(dp):
        rows = nt(whole[i * size : (i + 1) * size], whole[i * size :])
        for j in range(dp - i):
            packed[at * size : (at + 1) * size] = rows[:, j * size : (j + 1) * size]
            at += 1
    if at * size < packed.shape[0]:
        packed[at * size :] = jnp.zeros((packed.shape[0] - at * size, size), f32)
    count = packed.shape[0] // (nten * npre)
    for to, out in enumerate(outs):
        for by in range(npre):
            out[by * count : (by + 1) * count] = packed[rows_at((ten ^ to) * npre + (pre ^ by), count)]


def output_rows(dp, nb, npre, me, pre, count, width):
    each, share = width // (dp * npre), dp // nb
    made = lax.broadcasted_iota(jnp.int32, (count, width), 0)
    column = lax.broadcasted_iota(jnp.int32, (count, width), 1)
    target = lax.rem(me, share) * nb + ((me // share) ^ (made // each))
    return ((target * npre + pre) * each + lax.rem(made, each) == column).astype(f32)


def normed_kernel(nb, npre, where, own, *refs):
    received, (normed, high, low, columns) = refs[:-4], refs[-4:]
    me, pre = where[0], where[2]
    size, dp = own.shape[0], len(received) + 1
    normed[rows_at(me, size)] = own[...].astype(bf16)
    for by, piece in enumerate(received, 1):
        normed[rows_at(me ^ by, size)] = piece[...].astype(bf16)
    high[...], low[...] = halves(nt(normed[...], normed[...]))
    select = output_rows(dp, nb, npre, me, pre, columns.shape[0], normed.shape[1])
    columns[...] = nt(select.astype(bf16), normed[...]).astype(bf16)


def root_kernel(dp, nb, npre, nten, where, normed, high, low, columns, *refs):
    pieces, outs, packed, inner = refs[: nten * npre], refs[nten * npre : -2], refs[-2], refs[-1]
    me, ten, pre = where[0], where[1], where[2]
    for at, piece in enumerate(pieces):
        packed[rows_at((ten ^ at // npre) * npre + (pre ^ at % npre), piece.shape[0])] = piece[...]
    total, width = normed.shape
    size, at = total // dp, 0
    for i in range(dp):
        for j in range(i, dp):
            tile = packed[at * size : (at + 1) * size]
            inner[i * size : (i + 1) * size, j * size : (j + 1) * size] = tile
            if j > i:
                inner[j * size : (j + 1) * size, i * size : (i + 1) * size] = tile.T
            at += 1
    tokens_gram = high[...], low[...]
    both = inner[...] * (tokens_gram[0].astype(f32) + tokens_gram[1].astype(f32))
    power = jnp.sum(jnp.sum(both, axis=0, keepdims=True), axis=1, keepdims=True)
    scaling = 2.0 * (power / (float(total) * float(total)) / width + damping)
    damp = damping / scaling
    base = (5.0 - damp) / 4.0
    core = halves(inner[...] * (1.0 / (scaling * (float(total) * float(total)))))
    mixed = halves(product(tokens_gram, core))
    rows = nn(columns[...], core[0]) + nn(columns[...], core[1])

    def step(value, weight):
        return base * value - 0.25 * product(halves(value), mixed) + weight * rows

    weight = 0.25 * damp
    value = step(-rows, weight)
    for _ in range(3):
        weight = weight * base
        value = step(value, weight)
    weight = weight * base
    value = step(value, weight - 1.25)
    root = lax.rsqrt(jnp.sqrt(scaling))
    value = halves(value * (0.25 * root))
    alone = (5.0 * base - damp * base * base * base * base * base) * 0.25 * root
    made = nn(value[0], normed[...]) + nn(value[1], normed[...])
    made = made + alone * output_rows(dp, nb, npre, me, pre, made.shape[0], width)
    each = outs[0].shape[0]
    for by, out in enumerate(outs):
        out[...] = made[by * each : (by + 1) * each]


def program(tokens, gain, cotangent):
    dp, nten, npre = (lax.axis_size(name) for name in ("dp", "tensor", "precond"))
    me, ten, pre = (lax.axis_index(name) for name in ("dp", "tensor", "precond"))
    where = jnp.stack([me, ten, pre]).astype(jnp.int32)
    size, width = tokens.shape
    total = size * dp
    nb = width // BLK
    share = dp // nb
    assert nb * BLK == width and share * nb == dp
    assert all(n & (n - 1) == 0 for n in (dp, nten, npre))
    hidden = cotangent.shape[1] // (nten * dp)
    assert hidden * nten * dp == cotangent.shape[1]

    def cotangent_part(to):
        return lax.dynamic_slice_in_dim(cotangent, (ten * dp + to) * hidden, hidden, 1)

    cotangents = [swap(cotangent_part(me ^ by).astype(f32), "dp", by) for by in range(1, dp)]
    cotangents = [cotangent_part(me)] + cotangents

    values = tokens.astype(f32)
    square = jnp.sum(values * values, axis=1)[None, :]
    square = square + sum(swap(square, "tensor", by) for by in range(1, nten))
    inverse = lax.rsqrt(square[0][:, None] / (width * nten) + epsilon)

    def normed_part(to):
        at = (to // share) * BLK
        part = lax.dynamic_slice_in_dim(tokens, at, BLK, 1).astype(f32)
        scale = lax.dynamic_slice_in_dim(gain, at, BLK, 0).astype(f32)
        return part * inverse * scale

    normed_parts = [normed_part(me)]
    for by in range(1, dp):
        normed_parts.append(swap(normed_part(me ^ by), "dp", by))

    tiles = dp * (dp + 1) // 2
    piece = -(-tiles * size // (nten * npre * 8)) * 8
    packed = pltpu.VMEM((nten * npre * piece, size), f32)
    part = jax.ShapeDtypeStruct((npre * piece, size), f32)
    parts = call(
        functools.partial(gram_kernel, nten, npre),
        [part] * nten,
        where,
        *cotangents,
        scratch=[pltpu.VMEM((total, hidden), bf16), packed],
        flops=tiles * size * size * hidden * 2,
    )
    part = parts[0] + sum(swap(parts[to], "tensor", to) for to in range(1, nten))
    summed = part[:piece] + sum(
        swap(part[by * piece : (by + 1) * piece], "precond", by) for by in range(1, npre)
    )
    summed = summed + sum(swap(summed, "dp", by) for by in range(1, dp))
    pieces = [summed] + [swap(summed, "precond", by) for by in range(1, npre)]
    pieces = pieces + [swap(one, "tensor", to) for to in range(1, nten) for one in pieces]

    each = BLK // (dp * npre)
    made = nb * each
    normed, high, low, columns = call(
        functools.partial(normed_kernel, nb, npre),
        [
            jax.ShapeDtypeStruct((total, BLK), bf16),
            jax.ShapeDtypeStruct((total, total), bf16),
            jax.ShapeDtypeStruct((total, total), bf16),
            jax.ShapeDtypeStruct((made, total), bf16),
        ],
        where,
        *normed_parts,
        flops=2 * total * total * BLK + 2 * made * BLK * total,
    )
    rows = call(
        functools.partial(root_kernel, dp, nb, npre, nten),
        [jax.ShapeDtypeStruct((each, BLK), f32)] * nb,
        where,
        normed,
        high,
        low,
        columns,
        *pieces,
        scratch=[packed, pltpu.VMEM((total, total), f32)],
        flops=2 * total * total * (3 * total + 17 * made),
    )
    result = jnp.zeros((nb, each, BLK), f32)
    for by in range(nb):
        pairs = [(b * share + m, m * nb + (b ^ by)) for b in range(nb) for m in range(share)]
        sent = rows[by]
        if any(a != b for a, b in pairs):
            sent = lax.ppermute(sent, "dp", pairs)
        result = lax.dynamic_update_slice_in_dim(result, sent[None], lax.rem(me, nb) ^ by, 0)
    return result


def solution(mesh):
    in_specs = (P("dp", "tensor"), P("tensor"), P("dp", "precond"))
    out_specs = P("tensor", ("dp", "precond"), None)
    return jax.shard_map(program, mesh=mesh, in_specs=in_specs, out_specs=out_specs, check_vma=False)
```

```python
import functools

import jax
import jax.numpy as jnp
from jax import lax
from jax.experimental import pallas as pl
from jax.experimental.pallas import tpu as pltpu
from jax.sharding import PartitionSpec as P

BLK = 1024


epsilon = 1e-06
damping = 0.01

f32 = jnp.float32
bf16 = jnp.bfloat16
VMEM = pl.BlockSpec(memory_space=pltpu.VMEM)
ANY = pl.BlockSpec(memory_space=pl.ANY)
SMEM = pl.BlockSpec(memory_space=pltpu.SMEM)


def swap(value, axis, by):
    size = lax.axis_size(axis)
    return lax.ppermute(value, axis, [(i, i ^ by) for i in range(size)])


def call(kernel, outs, *operands, scratch=(), flops=0, vmem=16, out_spec=VMEM):
    moved = sum(a.size * a.dtype.itemsize for a in (*operands, *outs))
    return pl.pallas_call(
        kernel,
        out_shape=list(outs),
        in_specs=[SMEM] + [VMEM] * (len(operands) - 1),
        out_specs=[out_spec] * len(outs),
        scratch_shapes=list(scratch),
        compiler_params=pltpu.CompilerParams(vmem_limit_bytes=vmem * 2**20),
        cost_estimate=pl.CostEstimate(flops=flops, bytes_accessed=moved, transcendentals=0),
    )(*operands)


def nt(left, right):
    return lax.dot_general(left, right, (((1,), (1,)), ((), ())), preferred_element_type=f32)


def nn(left, right):
    return lax.dot_general(left, right, (((1,), (0,)), ((), ())), preferred_element_type=f32)


def halves(value):
    high = value.astype(bf16)
    return high, (value - high.astype(f32)).astype(bf16)


def twice(left, right):
    count = left[0].shape[0]
    both = nn(jnp.concatenate(left, axis=0), right)
    return both[:count] + both[count:]


def product(left, right):
    return twice(left, right[0]) + nn(left[0], right[1])


def rows_at(index, count):
    return pl.ds(pl.multiple_of(index * count, 8), count)


def positions(size):
    return tuple(lax.broadcasted_iota(jnp.int32, (size, size), axis) for axis in (0, 1))


def packed_rows(dp, size):
    return dp // 2 * size + dp * (dp - 1) // 2 * size + 8


def gram_kernel(nten, npre, where, own, *refs):
    received, outs, whole, packed = refs[: -nten - 2], refs[-nten - 2 : -2], refs[-2], refs[-1]
    me, ten, pre = where[0], where[1], where[2]
    size, dp = own.shape[0], len(received) + 1
    whole[rows_at(me, size)] = own[...].astype(bf16)
    for by, piece in enumerate(received, 1):
        whole[rows_at(me ^ by, size)] = piece[...].astype(bf16)
    down, across = positions(size)
    even, at = None, dp // 2 * size
    packed[packed_rows(dp, size) - 8 :] = jnp.zeros((packed.shape[0] - packed_rows(dp, size) + 8, size), f32)
    for i in range(dp):
        rows = nt(whole[i * size : (i + 1) * size], whole[i * size :])
        if i % 2 == 0:
            even = rows[:, :size]
        else:
            pair = i // 2
            packed[pair * size : (pair + 1) * size] = jnp.where(across >= down, even, rows[:, :size])
            spare = packed_rows(dp, size) - 8 + pair
            packed[spare : spare + 1] = jnp.sum(
                jnp.where(across == down, rows[:, :size], 0.0), axis=0, keepdims=True
            )
        for j in range(1, dp - i):
            packed[at : at + size] = rows[:, j * size : (j + 1) * size]
            at += size
    count = packed.shape[0] // (nten * npre)
    for to, out in enumerate(outs):
        for by in range(npre):
            out[by * count : (by + 1) * count] = packed[rows_at((ten ^ to) * npre + (pre ^ by), count)]


def output_rows(dp, nb, npre, me, pre, count, width):
    each, share = width // (dp * npre), dp // nb
    made = lax.broadcasted_iota(jnp.int32, (count, width), 0)
    column = lax.broadcasted_iota(jnp.int32, (count, width), 1)
    target = lax.rem(me, share) * nb + ((me // share) ^ (made // each))
    return ((target * npre + pre) * each + lax.rem(made, each) == column).astype(f32)


def normed_kernel(nb, npre, where, own, *refs):
    received, (normed, high, low, columns) = refs[:-4], refs[-4:]
    me, pre = where[0], where[2]
    size, dp = own.shape[0], len(received) + 1
    normed[rows_at(me, size)] = own[...].astype(bf16)
    for by, piece in enumerate(received, 1):
        normed[rows_at(me ^ by, size)] = piece[...].astype(bf16)
    high[...], low[...] = halves(nt(normed[...], normed[...]))
    select = output_rows(dp, nb, npre, me, pre, columns.shape[0], normed.shape[1])
    columns[...] = nt(select.astype(bf16), normed[...]).astype(bf16)


def root_kernel(dp, nb, npre, nten, where, normed, high, low, columns, *refs):
    pieces, outs, packed, inner = refs[: nten * npre], refs[nten * npre : -2], refs[-2], refs[-1]
    me, ten, pre = where[0], where[1], where[2]
    for at, piece in enumerate(pieces):
        packed[rows_at((ten ^ at // npre) * npre + (pre ^ at % npre), piece.shape[0])] = piece[...]
    total, width = normed.shape
    size = total // dp
    at = dp // 2 * size
    down, across = positions(size)
    for i in range(dp):
        pair = i // 2
        tile = packed[pair * size : (pair + 1) * size]
        turned = tile.T
        if i % 2 == 0:
            tile = jnp.where(across >= down, tile, turned)
        else:
            spare = packed_rows(dp, size) - 8 + pair
            tile = jnp.where(across < down, tile, turned)
            tile = jnp.where(across == down, packed[spare : spare + 1], tile)
        inner[i * size : (i + 1) * size, i * size : (i + 1) * size] = tile
        for j in range(i + 1, dp):
            tile = packed[at : at + size]
            inner[i * size : (i + 1) * size, j * size : (j + 1) * size] = tile
            inner[j * size : (j + 1) * size, i * size : (i + 1) * size] = tile.T
            at += size
    tokens_gram = high[...], low[...]
    both = inner[...] * (tokens_gram[0].astype(f32) + tokens_gram[1].astype(f32))
    power = jnp.sum(jnp.sum(both, axis=0, keepdims=True), axis=1, keepdims=True)
    scaling = 2.0 * (power / (float(total) * float(total)) / width + damping)
    damp = damping / scaling
    base = (5.0 - damp) / 4.0
    core = halves(inner[...] * (1.0 / (scaling * (float(total) * float(total)))))
    mixed = halves(product(tokens_gram, core))
    rows = nn(columns[...], core[0]) + nn(columns[...], core[1])

    def step(value, weight):
        return base * value - 0.25 * product(halves(value), mixed) + weight * rows

    weight = 0.25 * damp
    value = step(-rows, weight)
    for _ in range(3):
        weight = weight * base
        value = step(value, weight)
    weight = weight * base
    value = step(value, weight - 1.25)
    root = lax.rsqrt(jnp.sqrt(scaling))
    value = halves(value * (0.25 * root))
    alone = (5.0 * base - damp * base * base * base * base * base) * 0.25 * root
    made = twice(value, normed[...])
    made = made + alone * output_rows(dp, nb, npre, me, pre, made.shape[0], width)
    each = outs[0].shape[0]
    for by, out in enumerate(outs):
        out[...] = made[by * each : (by + 1) * each]


def place_kernel(nb, where, *refs):
    parts, out, done = refs[:-2], refs[-2], refs[-1]
    here = lax.rem(where[0], nb)
    copies = [
        pltpu.make_async_copy(part, out.at[here ^ by], done.at[by]) for by, part in enumerate(parts)
    ]
    for copy in copies:
        copy.start()
    for copy in copies:
        copy.wait()


def program(tokens, gain, cotangent):
    dp, nten, npre = (lax.axis_size(name) for name in ("dp", "tensor", "precond"))
    me, ten, pre = (lax.axis_index(name) for name in ("dp", "tensor", "precond"))
    where = jnp.stack([me, ten, pre]).astype(jnp.int32)
    size, width = tokens.shape
    total = size * dp
    nb = width // BLK
    share = dp // nb
    assert nb * BLK == width and share * nb == dp
    assert all(n & (n - 1) == 0 for n in (dp, nten, npre)) and 2 <= dp <= 16
    hidden = cotangent.shape[1] // (nten * dp)
    assert hidden * nten * dp == cotangent.shape[1]

    def cotangent_part(to):
        return lax.dynamic_slice_in_dim(cotangent, (ten * dp + to) * hidden, hidden, 1)

    cotangents = [cotangent_part(me)]
    for by in range(1, dp):
        cotangents.append(swap(cotangent_part(me ^ by).astype(f32), "dp", by))

    values = tokens.astype(f32)
    square = jnp.sum(values * values, axis=1)[None, :]
    square = square + sum(swap(square, "tensor", by) for by in range(1, nten))
    inverse = lax.rsqrt(square[0][:, None] / (width * nten) + epsilon)

    def normed_part(to):
        at = (to // share) * BLK
        part = lax.dynamic_slice_in_dim(tokens, at, BLK, 1).astype(f32)
        scale = lax.dynamic_slice_in_dim(gain, at, BLK, 0).astype(f32)
        return part * inverse * scale

    normed_parts = [normed_part(me ^ by) for by in range(dp)]
    for by in range(1, dp):
        normed_parts[by] = swap(normed_parts[by], "dp", by)

    piece = -(-packed_rows(dp, size) // (nten * npre * 8)) * 8
    packed = pltpu.VMEM((nten * npre * piece, size), f32)
    part = jax.ShapeDtypeStruct((npre * piece, size), f32)
    parts = call(
        functools.partial(gram_kernel, nten, npre),
        [part] * nten,
        where,
        *cotangents,
        scratch=[pltpu.VMEM((total, hidden), bf16), packed],
        flops=total * total * hidden,
    )
    part = parts[0] + sum(swap(parts[to], "tensor", to) for to in range(1, nten))
    summed = part[:piece] + sum(
        swap(part[by * piece : (by + 1) * piece], "precond", by) for by in range(1, npre)
    )
    summed = summed + sum(swap(summed, "dp", by) for by in range(1, dp))
    pieces = [summed] + [swap(summed, "precond", by) for by in range(1, npre)]
    pieces = pieces + [swap(one, "tensor", to) for to in range(1, nten) for one in pieces]

    each = BLK // (dp * npre)
    made = nb * each
    normed, high, low, columns = call(
        functools.partial(normed_kernel, nb, npre),
        [
            jax.ShapeDtypeStruct((total, BLK), bf16),
            jax.ShapeDtypeStruct((total, total), bf16),
            jax.ShapeDtypeStruct((total, total), bf16),
            jax.ShapeDtypeStruct((made, total), bf16),
        ],
        where,
        *normed_parts,
        flops=2 * total * total * BLK + 2 * made * BLK * total,
    )
    rows = call(
        functools.partial(root_kernel, dp, nb, npre, nten),
        [jax.ShapeDtypeStruct((each, BLK), f32)] * nb,
        where,
        normed,
        high,
        low,
        columns,
        *pieces,
        scratch=[packed, pltpu.VMEM((total, total), f32)],
        flops=2 * total * total * (3 * total + 17 * made),
    )
    rows = list(rows)
    for by in range(nb):
        pairs = [(b * share + m, m * nb + (b ^ by)) for b in range(nb) for m in range(share)]
        if any(a != b for a, b in pairs):
            rows[by] = lax.ppermute(rows[by], "dp", pairs)
    last = 1
    (result,) = call(
        functools.partial(place_kernel, nb),
        [jax.ShapeDtypeStruct((nb, each, BLK), f32)],
        where,
        *rows[:last],
        scratch=[pltpu.SemaphoreType.DMA((last,))],
        vmem=4,
        out_spec=ANY,
    )
    for by in range(last, nb):
        result = lax.dynamic_update_slice_in_dim(result, rows[by][None], lax.rem(me, nb) ^ by, 0)
    return result


def solution(mesh):
    in_specs = (P("dp", "tensor"), P("tensor"), P("dp", "precond"))
    out_specs = P("tensor", ("dp", "precond"), None)
    return jax.shard_map(program, mesh=mesh, in_specs=in_specs, out_specs=out_specs, check_vma=False)
```

```python
import functools

import jax
import jax.numpy as jnp
from jax import lax
from jax.experimental import pallas as pl
from jax.experimental.pallas import tpu as pltpu
from jax.sharding import PartitionSpec as P

BLK = 1024


epsilon = 1e-06
damping = 0.01

f32 = jnp.float32
bf16 = jnp.bfloat16
VMEM = pl.BlockSpec(memory_space=pltpu.VMEM)
ANY = pl.BlockSpec(memory_space=pl.ANY)
SMEM = pl.BlockSpec(memory_space=pltpu.SMEM)


def swap(value, axis, by, named=False):
    size = lax.axis_size(axis)
    if named:
        return swap(value, axis, by)
    return lax.ppermute(value, axis, [(i, i ^ by) for i in range(size)])


def call(kernel, outs, *operands, scratch=(), flops=0, vmem=16, out_spec=VMEM):
    moved = sum(a.size * a.dtype.itemsize for a in (*operands, *outs))
    return pl.pallas_call(
        kernel,
        out_shape=list(outs),
        in_specs=[SMEM] + [VMEM] * (len(operands) - 1),
        out_specs=[out_spec] * len(outs),
        scratch_shapes=list(scratch),
        compiler_params=pltpu.CompilerParams(vmem_limit_bytes=vmem * 2**20),
        cost_estimate=pl.CostEstimate(flops=flops, bytes_accessed=moved, transcendentals=0),
    )(*operands)


def nt(left, right):
    return lax.dot_general(left, right, (((1,), (1,)), ((), ())), preferred_element_type=f32)


def nn(left, right):
    return lax.dot_general(left, right, (((1,), (0,)), ((), ())), preferred_element_type=f32)


def halves(value):
    high = value.astype(bf16)
    return high, (value - high.astype(f32)).astype(bf16)


def twice(left, right):
    count = left[0].shape[0]
    both = nn(jnp.concatenate(left, axis=0), right)
    return both[:count] + both[count:]


def product(left, right):
    return twice(left, right[0]) + nn(left[0], right[1])


def rows_at(index, count):
    return pl.ds(pl.multiple_of(index * count, 8), count)


def positions(size):
    return tuple(lax.broadcasted_iota(jnp.int32, (size, size), axis) for axis in (0, 1))


def packed_rows(dp, size):
    return dp // 2 * size + dp * (dp - 1) // 2 * size + 8


def gram_kernel(nten, npre, where, own, *refs):
    received, outs, whole, packed = refs[: -nten - 2], refs[-nten - 2 : -2], refs[-2], refs[-1]
    me, ten, pre = where[0], where[1], where[2]
    size, dp = own.shape[0], len(received) + 1
    whole[rows_at(me, size)] = own[...].astype(bf16)
    for by, piece in enumerate(received, 1):
        whole[rows_at(me ^ by, size)] = piece[...].astype(bf16)
    down, across = positions(size)
    even, at = None, dp // 2 * size
    packed[packed_rows(dp, size) - 8 :] = jnp.zeros((packed.shape[0] - packed_rows(dp, size) + 8, size), f32)
    for i in range(dp):
        rows = nt(whole[i * size : (i + 1) * size], whole[i * size :])
        if i % 2 == 0:
            even = rows[:, :size]
        else:
            pair = i // 2
            packed[pair * size : (pair + 1) * size] = jnp.where(across >= down, even, rows[:, :size])
            spare = packed_rows(dp, size) - 8 + pair
            packed[spare : spare + 1] = jnp.sum(
                jnp.where(across == down, rows[:, :size], 0.0), axis=0, keepdims=True
            )
        for j in range(1, dp - i):
            packed[at : at + size] = rows[:, j * size : (j + 1) * size]
            at += size
    count = packed.shape[0] // (nten * npre)
    for to, out in enumerate(outs):
        for by in range(npre):
            out[by * count : (by + 1) * count] = packed[rows_at((ten ^ to) * npre + (pre ^ by), count)]


def output_rows(dp, nb, npre, me, pre, count, width):
    each, share = width // (dp * npre), dp // nb
    made = lax.broadcasted_iota(jnp.int32, (count, width), 0)
    column = lax.broadcasted_iota(jnp.int32, (count, width), 1)
    target = lax.rem(me, share) * nb + ((me // share) ^ (made // each))
    return ((target * npre + pre) * each + lax.rem(made, each) == column).astype(f32)


def early_kernel(dp, nb, npre, where, *refs):
    received, (normed, high, low, columns) = refs[:-4], refs[-4:]
    size = received[0].shape[0]
    for at, piece in enumerate(received):
        normed[at * size : (at + 1) * size] = piece[...].astype(bf16)
    high[...], low[...] = halves(nt(normed[...], normed[...]))
    select = output_rows(dp, nb, npre, where[0], where[2], columns.shape[0], normed.shape[1])
    columns[...] = nt(select.astype(bf16), normed[...]).astype(bf16)


def root_kernel(dp, nb, npre, nten, order, where, old, high, low, columns, *refs):
    fresh = refs[: dp - old.shape[0] // refs[0].shape[0]]
    refs = refs[len(fresh) :]
    pieces, outs, (packed, inner, normed) = refs[: nten * npre], refs[nten * npre : -3], refs[-3:]
    me, ten, pre = where[0], where[1], where[2]
    size, first = fresh[0].shape[0], old.shape[0]
    total, width = normed.shape
    normed[:first] = old[...]
    for at, piece in enumerate(fresh):
        normed[first + at * size : first + (at + 1) * size] = piece[...].astype(bf16)
    for at, piece in enumerate(pieces):
        packed[rows_at((ten ^ at // npre) * npre + (pre ^ at % npre), piece.shape[0])] = piece[...]

    def place(i):
        return sum(jnp.where(me ^ i == by, at, 0) for at, by in enumerate(order))

    places = [place(i) for i in range(dp)]
    spot = [pl.ds(pl.multiple_of(at * size, size), size) for at in places]
    at = dp // 2 * size
    down, across = positions(size)
    for i in range(dp):
        pair = i // 2
        tile = packed[pair * size : (pair + 1) * size]
        turned = tile.T
        if i % 2 == 0:
            tile = jnp.where(across >= down, tile, turned)
        else:
            spare = packed_rows(dp, size) - 8 + pair
            tile = jnp.where(across < down, tile, turned)
            tile = jnp.where(across == down, packed[spare : spare + 1], tile)
        inner[spot[i], spot[i]] = tile
        for j in range(i + 1, dp):
            tile = packed[at : at + size]
            inner[spot[i], spot[j]] = tile
            inner[spot[j], spot[i]] = tile.T
            at += size
    select = output_rows(dp, nb, npre, me, pre, columns.shape[0], width)
    later = normed[first:]
    left = jnp.concatenate([columns[...], nt(select.astype(bf16), later).astype(bf16)], axis=1)
    upper = halves(nt(normed[:first], later))
    lower = halves(nt(later, normed[...]))
    tokens_gram = [
        jnp.concatenate([jnp.concatenate([one[...], two], axis=1), three], axis=0)
        for one, two, three in zip((high, low), upper, lower)
    ]
    both = inner[...] * (tokens_gram[0].astype(f32) + tokens_gram[1].astype(f32))
    power = jnp.sum(jnp.sum(both, axis=0, keepdims=True), axis=1, keepdims=True)
    scaling = 2.0 * (power / (float(total) * float(total)) / width + damping)
    damp = damping / scaling
    base = (5.0 - damp) / 4.0
    scale = 1.0 / (scaling * (float(total) * float(total)))
    core = halves(inner[...])
    mixed = halves(product(tokens_gram, core) * scale)
    rows = (nn(left, core[0]) + nn(left, core[1])) * scale

    def step(value, weight):
        return base * value - 0.25 * product(halves(value), mixed) + weight * rows

    weight = 0.25 * damp
    value = step(-rows, weight)
    for _ in range(3):
        weight = weight * base
        value = step(value, weight)
    weight = weight * base
    value = step(value, weight - 1.25)
    root = lax.rsqrt(jnp.sqrt(scaling))
    value = halves(value * (0.25 * root))
    alone = (5.0 * base - damp * base * base * base * base * base) * 0.25 * root
    made = twice(value, normed[...]) + alone * select
    each = outs[0].shape[0]
    for by, out in enumerate(outs):
        out[...] = made[by * each : (by + 1) * each]


def place_kernel(nb, where, *refs):
    parts, out, done = refs[:-2], refs[-2], refs[-1]
    here = lax.rem(where[0], nb)
    copies = [
        pltpu.make_async_copy(part, out.at[here ^ by], done.at[by]) for by, part in enumerate(parts)
    ]
    for copy in copies:
        copy.start()
    for copy in copies:
        copy.wait()


def program(tokens, gain, cotangent):
    dp, nten, npre = (lax.axis_size(name) for name in ("dp", "tensor", "precond"))
    me, ten, pre = (lax.axis_index(name) for name in ("dp", "tensor", "precond"))
    where = jnp.stack([me, ten, pre]).astype(jnp.int32)
    size, width = tokens.shape
    total = size * dp
    nb = width // BLK
    share = dp // nb
    assert nb * BLK == width and share * nb == dp
    assert all(n & (n - 1) == 0 for n in (dp, nten, npre)) and 2 <= dp <= 16
    hidden = cotangent.shape[1] // (nten * dp)
    assert hidden * nten * dp == cotangent.shape[1]

    def cotangent_part(to):
        return lax.dynamic_slice_in_dim(cotangent, (ten * dp + to) * hidden, hidden, 1)

    cotangents = [cotangent_part(me)]
    for by in range(1, dp):
        cotangents.append(swap(cotangent_part(me ^ by).astype(f32), "dp", by))

    values = tokens.astype(f32)
    square = jnp.sum(values * values, axis=1)[None, :]
    square = square + sum(swap(square, "tensor", by) for by in range(1, nten))
    inverse = lax.rsqrt(square[0][:, None] / (width * nten) + epsilon)

    def normed_part(to):
        at = (to // share) * BLK
        part = lax.dynamic_slice_in_dim(tokens, at, BLK, 1).astype(f32)
        scale = lax.dynamic_slice_in_dim(gain, at, BLK, 0).astype(f32)
        return part * inverse * scale

    normed_parts = [normed_part(me ^ by) for by in range(dp)]
    for by in range(1, dp):
        normed_parts[by] = swap(normed_parts[by], "dp", by)

    piece = -(-packed_rows(dp, size) // (nten * npre * 8)) * 8
    packed = pltpu.VMEM((nten * npre * piece, size), f32)
    part = jax.ShapeDtypeStruct((npre * piece, size), f32)
    parts = call(
        functools.partial(gram_kernel, nten, npre),
        [part] * nten,
        where,
        *cotangents,
        scratch=[pltpu.VMEM((total, hidden), bf16), packed],
        flops=total * total * hidden,
    )
    part = parts[0] + sum(swap(parts[to], "tensor", to) for to in range(1, nten))
    summed = part[:piece] + sum(swap(part[by * piece : (by + 1) * piece], "precond", by, True) for by in range(1, npre))
    summed = summed + sum(swap(summed, "dp", by) for by in range(1, dp))
    pieces = [summed] + [swap(summed, "precond", by, True) for by in range(1, npre)]
    pieces = pieces + [swap(one, "tensor", to) for to in range(1, nten) for one in pieces]

    each = BLK // (dp * npre)
    made = nb * each
    near = [by for by in range(1, dp) if by & (by - 1) == 0]
    early = [by for by in range(dp) if by not in near]
    first = len(early) * size
    old = call(
        functools.partial(early_kernel, dp, nb, npre),
        [
            jax.ShapeDtypeStruct((first, BLK), bf16),
            jax.ShapeDtypeStruct((first, first), bf16),
            jax.ShapeDtypeStruct((first, first), bf16),
            jax.ShapeDtypeStruct((made, first), bf16),
        ],
        where,
        *(normed_parts[by] for by in early),
        flops=2 * first * first * BLK + 2 * made * BLK * first,
    )
    rows = call(
        functools.partial(root_kernel, dp, nb, npre, nten, early + near),
        [jax.ShapeDtypeStruct((each, BLK), f32)] * nb,
        where,
        *old,
        *(normed_parts[by] for by in near),
        *pieces,
        scratch=[packed, pltpu.VMEM((total, total), f32), pltpu.VMEM((total, BLK), bf16)],
        flops=2 * total * total * (3 * total + 17 * made),
        vmem=20,
    )
    rows = list(rows)
    for by in range(nb):
        pairs = [(b * share + m, m * nb + (b ^ by)) for b in range(nb) for m in range(share)]
        if any(a != b for a, b in pairs):
            rows[by] = lax.ppermute(rows[by], "dp", pairs)
    last = 1
    (result,) = call(
        functools.partial(place_kernel, nb),
        [jax.ShapeDtypeStruct((nb, each, BLK), f32)],
        where,
        *rows[:last],
        scratch=[pltpu.SemaphoreType.DMA((last,))],
        vmem=4,
        out_spec=ANY,
    )
    for by in range(last, nb):
        result = lax.dynamic_update_slice_in_dim(result, rows[by][None], lax.rem(me, nb) ^ by, 0)
    return result


def solution(mesh):
    in_specs = (P("dp", "tensor"), P("tensor"), P("dp", "precond"))
    out_specs = P("tensor", ("dp", "precond"), None)
    return jax.shard_map(program, mesh=mesh, in_specs=in_specs, out_specs=out_specs, check_vma=False)
```
